32 devices in a mesh: groups: 2 (over x), seq: 8 (over z, y), head: 2 (over core).
Axes of the slice: x: 2, y: 2, z: 4, core: 2. Of those that a mesh axis runs over, the one named last changes fastest.
Arguments:
- queries: bfloat16 [4096, 32, 192], P(('groups', 'seq'), 'head'), parts along dimension 0, may hold values from -8 to 8
- keys: bfloat16 [4096, 4, 192], P(('groups', 'seq'), 'head'), parts along dimension 0, may hold values from -8 to 8
- values: bfloat16 [4096, 4, 128], P(('groups', 'seq'), 'head'), parts along dimension 0, may hold values from -6 to 6
- lists: int32 [64, 4, 16], P(('groups', 'seq'), 'head'), parts along dimension 0, may hold values from -1 to 31, as said below
- gate_weight: bfloat16 [32, 192, 3], P('head'), may hold values from -0.4375 to 0.4375
- pool_key: float32 [32, 4, 192], P(None, 'head'), may hold values from 0.08 to 0.3
- pool_value: float32 [32, 4, 128], P(None, 'head'), may hold values from 0.08 to 0.3
- out_weight: bfloat16 [2560, 4096], P(None, 'head'), may hold values from -0.09375 to 0.09375
Outputs:
- attended: bfloat16 [4096, 2560], P(('groups', 'seq'), 'head'), parts along dimension 0
The draws below stay inside these ranges and needn't reach their ends.
There are 2 independent parts, one for each index of `groups`. The reference program is written for one: setup_inputs(seed, part) draws one part's arguments, and reference() takes and returns one part's arrays. A program takes and returns all parts, laid end to end along the dimension named above; an argument that names none is the same for every part. Nothing has to cross between parts.
Inputs may be any that keep to these rules, and one draw needn't show every extreme that they name: `lists`: each entry is a block index of 64 tokens or -1 for an empty entry. The valid entries of one list are distinct, never lie after the tile's own block, and always include block 0, the tile's own block and the block before it. Over the tiles of one device's 256 tokens and one group, the valid entries that lie in any one other device's shard name at most 2 distinct blocks.
All inputs are finite; a program needn't handle non-finite values.
Results may differ from the reference program's by a relative error of at most 0.012.
Values may be sent and summed in bfloat16 or wider, within the bound.
No kernel may reach another device: no remote copies, remote signals or barrier semaphores. Data moves between devices by JAX's collectives and lax.ppermute only.
A program may use at most 192 MiB of HBM per device.

```python
import math
import jax
import jax.numpy as jnp
from jax import lax

D = 2560
HEADS = 32
GROUPS = 4
DQ = 192
DV = 128
BLOCK = 64
CBLOCK = 32
STRIDE = 16
TOP = 16
SLOTS = 2
WINDOW = 256
TOK_DEV = 256
HPG = 8
SEQLEN = 2048
NTILES = 32
N_SEQ = 8


def draw_queries(key, part):
    shape = (SEQLEN, HEADS, DQ)
    base = jnp.clip(jax.random.normal(jax.random.fold_in(key, 1), shape, jnp.float32), -8.0, 8.0)
    return base.astype(jnp.bfloat16)


def draw_keys(key, part):
    shape = (SEQLEN, GROUPS, DQ)
    base = jnp.clip(jax.random.normal(jax.random.fold_in(key, 3), shape, jnp.float32), -8.0, 8.0)
    return base.astype(jnp.bfloat16)


def draw_lists(key, part):
    blocks_dev = TOK_DEV // BLOCK
    offs = jnp.arange(blocks_dev, dtype=jnp.int32)
    owners = jnp.arange(N_SEQ, dtype=jnp.int32)
    device_axis = owners[:, None, None, None]
    owner_axis = owners[None, None, :, None]
    pick_score = jax.random.randint(jax.random.fold_in(key, 11), (N_SEQ, GROUPS, N_SEQ, blocks_dev), 0, 1 << 12) * blocks_dev + offs
    pick_score = jnp.where((owner_axis == device_axis - 1) & (offs == blocks_dev - 1), 1 << 28, pick_score)
    pick_score = jnp.where((owner_axis == 0) & (offs == 0), 1 << 29, pick_score)
    ignored, slot_offs = lax.top_k(pick_score, SLOTS)
    allowed = (owner_axis * blocks_dev + slot_offs).reshape(N_SEQ, GROUPS, N_SEQ * SLOTS)
    tile = jnp.arange(NTILES, dtype=jnp.int32)
    device_of_tile = tile // blocks_dev
    local_of_tile = tile % blocks_dev
    table = allowed[device_of_tile]
    own_blocks = device_of_tile[:, None] * blocks_dev + offs[None, :]
    own_blocks = jnp.broadcast_to(own_blocks[:, None, :], (NTILES, GROUPS, blocks_dev))
    candidate = jnp.concatenate([table, own_blocks], 2)
    width = N_SEQ * SLOTS + blocks_dev
    column = jnp.arange(width, dtype=jnp.int32)[None, None, :]
    usable = jnp.where(column < N_SEQ * SLOTS, column // SLOTS < device_of_tile[:, None, None], column - N_SEQ * SLOTS <= local_of_tile[:, None, None])
    noise = jax.random.randint(jax.random.fold_in(key, 12), (NTILES, GROUPS, width), 0, 1 << 16)
    here = tile[:, None, None]
    forced = (candidate == 0) | (candidate == here) | (candidate == here - 1)
    score = jnp.where(forced, 1 << 20, noise) * width + column
    score = jnp.where(usable, score, -1 - column)
    ignored, chosen = lax.top_k(score, TOP)
    okay = jnp.take_along_axis(usable, chosen, axis=2)
    block = jnp.take_along_axis(candidate, chosen, axis=2)
    return jnp.where(okay, block, -1).astype(jnp.int32)


def shard_levels(stream_key, extent, shards, smallest, largest):
    def one(axis_at, blocks):
        heights = jax.random.uniform(jax.random.fold_in(jax.random.fold_in(stream_key, 6), axis_at), (blocks,), jnp.float32, smallest / len(shards), largest / len(shards))
        return jnp.repeat(jnp.exp(heights), extent[axis_at] // blocks).reshape((-1,) + (1,) * (len(extent) - axis_at - 1))

    gain = one(*shards[0])
    for cut in shards[1:]:
        gain = gain * one(*cut)
    return gain


def normal_values(stream_key, shape, scale, most, cuts=(), held_as=jnp.bfloat16):
    drawn = jax.random.normal(stream_key, shape, jnp.float32) * scale
    if len(cuts) > 0:
        drawn = shard_levels(stream_key, shape, cuts, -0.22, 0.18) * drawn
    return jnp.clip(drawn, min=-most, max=most).astype(held_as)


def setup_inputs(seed: int = 0, part: int = 0) -> dict:
    streams_of = jax.random.split(jax.random.key(seed), 9)
    part_keys = jax.random.split(jax.random.fold_in(streams_of[8], part), 9)
    return {
        "queries": draw_queries(jax.random.fold_in(jax.random.fold_in(streams_of[8], part), 71), part),
        "keys": draw_keys(jax.random.fold_in(jax.random.fold_in(streams_of[8], part), 71), part),
        "values": normal_values(part_keys[2], (SEQLEN, GROUPS, DV), 1.0, 6.0, ((0, 8), (1, 2))),
        "lists": draw_lists(jax.random.fold_in(jax.random.fold_in(streams_of[8], part), 71), part),
        "gate_weight": normal_values(streams_of[4], (HEADS, DQ, 3), DQ ** -0.5, 0.4375, ((0, 2),)),
        "pool_key": jnp.clip(jnp.exp(math.log(0.3) - 1.3217559 * jax.random.uniform(streams_of[5], (CBLOCK, GROUPS, DQ), jnp.float32) ** shard_levels(streams_of[5], (CBLOCK, GROUPS, DQ), ((1, 2),), -0.2, 0.2)), 0.08, 0.3),
        "pool_value": jnp.clip(jnp.exp(math.log(0.3) - 1.3217559 * jax.random.uniform(streams_of[6], (CBLOCK, GROUPS, DV), jnp.float32) ** shard_levels(streams_of[6], (CBLOCK, GROUPS, DV), ((1, 2),), -0.2, 0.2)), 0.08, 0.3),
        "out_weight": normal_values(streams_of[7], (D, HEADS * DV), (HEADS * DV) ** -0.5, 0.09375, ((1, 2),)),
    }


def masked_weights(scores, mask):
    peak = jnp.max(jnp.where(mask, scores, -1e30), axis=-1, keepdims=True)
    raised = jnp.exp(jnp.where(mask, scores - peak, -1e30))
    total = jnp.sum(raised, axis=-1, keepdims=True)
    return (raised / jnp.maximum(total, 1.0)).astype(jnp.bfloat16)


def compress(raw, pool):
    count = raw.shape[0] // STRIDE
    tail = jnp.zeros((CBLOCK - STRIDE,) + raw.shape[1:], jnp.float32)
    padded = jnp.concatenate([raw.astype(jnp.float32), tail], 0)
    total = jnp.zeros((count,) + raw.shape[1:], jnp.float32)
    for part in range(CBLOCK // STRIDE):
        piece = padded[part * STRIDE:part * STRIDE + count * STRIDE].reshape((count, STRIDE) + raw.shape[1:])
        weights = pool[part * STRIDE:(part + 1) * STRIDE].astype(jnp.float32)
        total = total + jnp.einsum("csgd,sgd->cgd", piece, weights, precision=lax.Precision.HIGHEST)
    return total.astype(jnp.bfloat16)


def reference(queries, keys, values, lists, gate_weight, pool_key, pool_value, out_weight):
    length = queries.shape[0]
    scale = DQ ** -0.5
    q_rows = 512 if length % 512 == 0 else BLOCK
    tiles = q_rows // BLOCK
    comp_keys = compress(keys, pool_key).astype(jnp.float32)
    comp_values = compress(values, pool_value).astype(jnp.float32)
    comp_end = jnp.arange(comp_keys.shape[0], dtype=jnp.int32) * STRIDE + CBLOCK - 1
    front_k = jnp.zeros((WINDOW,) + keys.shape[1:], keys.dtype)
    front_v = jnp.zeros((WINDOW,) + values.shape[1:], values.dtype)
    pad_keys = jnp.concatenate([front_k, keys], 0)
    pad_values = jnp.concatenate([front_v, values], 0)
    gates = jax.nn.sigmoid(jnp.einsum("thd,hdb->thb", queries.astype(jnp.float32), gate_weight.astype(jnp.float32)))
    group_index = jnp.arange(GROUPS, dtype=jnp.int32)[None, :, None, None]
    offsets = jnp.arange(BLOCK, dtype=jnp.int32)

    def one_block(index):
        first = index * q_rows
        query = lax.dynamic_slice_in_dim(queries, first, q_rows, 0).astype(jnp.float32).reshape(q_rows, GROUPS, HPG, DQ)
        where_q = first + jnp.arange(q_rows, dtype=jnp.int32)
        scores = jnp.einsum("tghd,cgd->tghc", query, comp_keys) * scale
        mask = (comp_end[None, :] <= where_q[:, None])[:, None, None, :]
        weights = masked_weights(scores, mask)
        branch_c = jnp.einsum("tghc,cgd->tghd", weights.astype(jnp.float32), comp_values)

        listed = lax.dynamic_slice_in_dim(lists, index * tiles, tiles, 0)
        valid = listed >= 0
        rows = jnp.maximum(listed, 0)[..., None] * BLOCK + offsets
        chosen_keys = keys[rows, group_index].astype(jnp.float32)
        chosen_values = values[rows, group_index].astype(jnp.float32)
        tile_query = query.reshape(tiles, BLOCK, GROUPS, HPG, DQ)
        scores = jnp.einsum("atghd,agkrd->atghkr", tile_query, chosen_keys) * scale
        tile_where = where_q.reshape(tiles, BLOCK)
        mask = valid[:, None, :, None, :, None] & (rows[:, None, :, None, :, :] <= tile_where[:, :, None, None, None, None])
        scores = scores.reshape(tiles, BLOCK, GROUPS, HPG, TOP * BLOCK)
        mask = jnp.broadcast_to(mask, (tiles, BLOCK, GROUPS, 1, TOP, BLOCK)).reshape(tiles, BLOCK, GROUPS, 1, TOP * BLOCK)
        weights = masked_weights(scores, mask)
        branch_s = jnp.einsum("atghn,agnd->atghd", weights.astype(jnp.float32), chosen_values.reshape(tiles, GROUPS, TOP * BLOCK, DV))
        branch_s = branch_s.reshape(q_rows, GROUPS, HPG, DV)

        near_keys = lax.dynamic_slice_in_dim(pad_keys, first, WINDOW + q_rows, 0).astype(jnp.float32)
        near_values = lax.dynamic_slice_in_dim(pad_values, first, WINDOW + q_rows, 0).astype(jnp.float32)
        where_k = first - WINDOW + jnp.arange(WINDOW + q_rows, dtype=jnp.int32)
        mask = (where_k[None, :] >= 0) & (where_k[None, :] <= where_q[:, None]) & (where_k[None, :] > where_q[:, None] - WINDOW)
        scores = jnp.einsum("tghd,kgd->tghk", query, near_keys) * scale
        weights = masked_weights(scores, mask[:, None, None, :])
        branch_w = jnp.einsum("tghk,kgd->tghd", weights.astype(jnp.float32), near_values)

        gate = lax.dynamic_slice_in_dim(gates, first, q_rows, 0).reshape(q_rows, GROUPS, HPG, 3)
        mixed = gate[..., 0:1] * branch_c + gate[..., 1:2] * branch_s + gate[..., 2:3] * branch_w
        mixed = mixed.reshape(q_rows, HEADS * DV).astype(jnp.bfloat16)
        projected = lax.dot_general(mixed, out_weight, (((1,), (1,)), ((), ())), preferred_element_type=jnp.float32)
        return projected.astype(jnp.bfloat16)

    blocks = lax.map(one_block, jnp.arange(length // q_rows, dtype=jnp.int32))
    return blocks.reshape(length, out_weight.shape[0])
```

```python
import functools

import jax
import jax.numpy as jnp
from jax import lax
from jax.experimental import pallas as pl
from jax.experimental.pallas import tpu as pltpu
from jax.sharding import PartitionSpec as P

BLOCK = 64
CBLOCK = 32
STRIDE = 16
TOP = 16
WINDOW = 256
LANES = 128
LOW = -1e30


def inner_of(count):
    inner = 1
    while inner * inner * 2 < count and count % (inner * 2) == 0:
        inner *= 2
    return inner


def gather_shards(own, count):
    inner = inner_of(count)
    outer = count // inner
    index = lambda o, i: o * inner + i
    column = [own]
    for s in range(1, outer):
        pairs = [(index(o, i), index(o + 1, i)) for o in range(s - 1, outer - 1) for i in range(inner)]
        column.append(lax.ppermute(column[-1], "seq", pairs))
    slots = []
    for s in range(outer):
        slots.append(column[s])
        for k in range(1, inner):
            pairs = [
                (index(o, i), index(o, (i + k) % inner))
                for o in range(s, outer)
                for i in range(inner)
                if s > 0 or i + k < inner
            ]
            slots.append(lax.ppermute(column[s], "seq", pairs))
    return slots


def pack_kv(keys, values):
    rows, groups_dev, dk = keys.shape
    main = keys[:, :, :LANES].reshape(rows, -1)
    tail = keys[:, :, LANES:].reshape(rows, -1)
    return jnp.concatenate([main, tail, values.reshape(rows, -1)], axis=1)


def kernel(
    dims, place_ref, lists_ref, q_ref, gates_ref, spots_ref, pool_ref, *rest
):
    count, inner, rows_dev, groups_dev, per_group, tail, dv = dims
    slot_refs = rest[:count]
    mixed_ref, kv, front, back, comp, sems = rest[count:]
    width = kv.shape[1]
    main_w = groups_dev * LANES
    tail_w = groups_dev * tail
    value_at = main_w + tail_w
    tiles = rows_dev // BLOCK
    blocks_dev = tiles
    comp_dev = rows_dev // STRIDE
    here = place_ref[0]
    here_o = here // inner
    here_i = here % inner
    copies = [
        pltpu.make_async_copy(ref, kv.at[pl.ds(n * rows_dev, rows_dev)], sems.at[n])
        for n, ref in enumerate(slot_refs)
    ]
    for copy in copies:
        copy.start()
    front[...] = jnp.zeros_like(front)
    back[...] = jnp.zeros_like(back)
    for copy in copies:
        copy.wait()

    def shard_row(shard):
        s = here_o - shard // inner
        k = lax.rem(here_i - lax.rem(shard, inner) + inner, inner)
        return (s * inner + k) * rows_dev

    def block_row(block):
        return pl.multiple_of(shard_row(block // blocks_dev) + lax.rem(block, blocks_dev) * BLOCK, BLOCK)

    @pl.loop(0, here + 1)
    def _(shard):
        row = pl.multiple_of(shard_row(shard), rows_dev)
        out = pl.multiple_of(shard * comp_dev, comp_dev)
        x = kv[pl.ds(row, rows_dev), :].astype(jnp.float32).reshape(comp_dev, STRIDE, width)
        front[pl.ds(out, comp_dev), :] = jnp.sum(x * pool_ref[:STRIDE, :][None], axis=1)
        back[pl.ds(out, comp_dev), :] = jnp.sum(x * pool_ref[STRIDE:, :][None], axis=1)

    comp_rows = comp.shape[0]
    comp[...] = (front[:comp_rows, :] + back[1 : comp_rows + 1, :]).astype(jnp.bfloat16)

    rows = per_group * BLOCK
    factor = (LANES + tail) ** (-0.5)

    def keys_of(ref, row, size, g):
        return jnp.concatenate(
            [ref[pl.ds(row, size), g * LANES : (g + 1) * LANES], ref[pl.ds(row, size), main_w : main_w + tail_w]], 1
        )

    def values_of(ref, row, size, g):
        return ref[pl.ds(row, size), value_at + g * dv : value_at + (g + 1) * dv]

    def branch(query, keys, values, mask, gate):
        scores = lax.dot_general(query, keys, (((1,), (1,)), ((), ())), preferred_element_type=jnp.float32)
        scores = jnp.where(mask, scores * factor, LOW)
        peak = jnp.maximum(jnp.max(scores, axis=1, keepdims=True), LOW * 0.1)
        raised = jnp.exp(scores - peak)
        total = jnp.sum(raised, axis=1, keepdims=True)
        out = jnp.dot(raised.astype(jnp.bfloat16), values, preferred_element_type=jnp.float32)
        return out * (gate / jnp.maximum(total, 1.0))

    @pl.loop(0, tiles)
    def _(tile):
        global_tile = here * blocks_dev + tile
        where_q = global_tile * BLOCK + lax.rem(lax.broadcasted_iota(jnp.int32, (rows, 1), 0), BLOCK)
        for g in range(groups_dev):
            query = q_ref[g, tile]
            gate = gates_ref[g, tile]
            comp_end = lax.broadcasted_iota(jnp.int32, (1, comp_rows), 1) * STRIDE + CBLOCK - 1
            acc = branch(query, keys_of(comp, 0, comp_rows, g), values_of(comp, 0, comp_rows, g), comp_end <= where_q, gate[:, 0:1])
            near = range(WINDOW // BLOCK + 1)
            starts = [block_row(jnp.maximum(global_tile - WINDOW // BLOCK + j, 0)) for j in near]
            where_k = (global_tile * BLOCK - WINDOW) + lax.broadcasted_iota(jnp.int32, (1, len(near) * BLOCK), 1)
            mask = (where_k <= where_q) & (where_k > where_q - WINDOW) & (where_k >= 0)
            acc += branch(
                query,
                jnp.concatenate([keys_of(kv, r, BLOCK, g) for r in starts], 0),
                jnp.concatenate([values_of(kv, r, BLOCK, g) for r in starts], 0),
                mask,
                gate[:, 2:3],
            )
            starts = [block_row(jnp.maximum(lists_ref[tile, g, j], 0)) for j in range(TOP)]
            acc += branch(
                query,
                jnp.concatenate([keys_of(kv, r, BLOCK, g) for r in starts], 0),
                jnp.concatenate([values_of(kv, r, BLOCK, g) for r in starts], 0),
                spots_ref[g, tile] <= where_q,
                gate[:, 1:2],
            )
            out_row = pl.multiple_of(tile * BLOCK, BLOCK)
            for h in range(per_group):
                c = (g * per_group + h) * dv
                mixed_ref[pl.ds(out_row, BLOCK), c : c + dv] = acc[h * BLOCK : (h + 1) * BLOCK].astype(jnp.bfloat16)


def shards(count, queries, keys, values, lists, gate_weight, pool_key, pool_value, out_weight):
    rows_dev, heads_dev, head_size = queries.shape
    groups_dev = keys.shape[1]
    per_group = heads_dev // groups_dev
    value_size = values.shape[2]
    tiles = lists.shape[0]
    tail = head_size - LANES
    inner = inner_of(count)
    slots = gather_shards(pack_kv(keys, values), count)
    width = slots[0].shape[1]
    here = lax.axis_index("seq").astype(jnp.int32)
    pool = pack_kv(pool_key, pool_value)
    gates = jax.nn.sigmoid(
        jnp.einsum("thd,hdb->htb", queries, gate_weight, preferred_element_type=jnp.float32)
    )

    def by_tile(x):
        x = x.reshape(groups_dev, per_group, tiles, BLOCK, x.shape[-1])
        return x.transpose(0, 2, 1, 3, 4).reshape(groups_dev, tiles, per_group * BLOCK, x.shape[-1])

    by_head = by_tile(queries.transpose(1, 0, 2))
    wide = jnp.stack(
        [
            jnp.concatenate(
                [
                    by_head[g, ..., :LANES],
                    jnp.pad(by_head[g, ..., LANES:], ((0, 0), (0, 0), (g * tail, (groups_dev - 1 - g) * tail))),
                ],
                -1,
            )
            for g in range(groups_dev)
        ]
    )
    spots = jnp.where(
        lists[..., None] >= 0, lists[..., None] * BLOCK + jnp.arange(BLOCK, dtype=jnp.int32), jnp.int32(1 << 30)
    )
    spots = spots.reshape(tiles, groups_dev, 1, TOP * BLOCK).transpose(1, 0, 2, 3)
    comp_rows = count * rows_dev // STRIDE
    vmem = pl.BlockSpec(memory_space=pltpu.VMEM)
    smem = pl.BlockSpec(memory_space=pltpu.SMEM)
    mixed = pl.pallas_call(
        functools.partial(kernel, (count, inner, rows_dev, groups_dev, per_group, tail, value_size)),
        out_shape=jax.ShapeDtypeStruct((rows_dev, heads_dev * value_size), jnp.bfloat16),
        in_specs=[smem, smem, vmem, vmem, vmem, vmem] + [pl.BlockSpec(memory_space=pl.ANY)] * count,
        out_specs=vmem,
        scratch_shapes=[
            pltpu.VMEM((count * rows_dev, width), jnp.bfloat16),
            pltpu.VMEM((comp_rows + 8, width), jnp.float32),
            pltpu.VMEM((comp_rows + 8, width), jnp.float32),
            pltpu.VMEM((comp_rows, width), jnp.bfloat16),
            pltpu.SemaphoreType.DMA((count,)),
        ],
        compiler_params=pltpu.CompilerParams(vmem_limit_bytes=60 * 1024 * 1024),
        cost_estimate=pl.CostEstimate(flops=10**10, bytes_accessed=10**7, transcendentals=10**7),
    )(here[None], lists, wide, by_tile(gates), spots, pool, *slots)
    half = out_weight.shape[0] // lax.axis_size("head")
    side = lax.axis_index("head")

    def project(which):
        weight = lax.dynamic_slice_in_dim(out_weight, which * half, half, 0)
        return lax.dot_general(mixed, weight, (((1,), (1,)), ((), ())), preferred_element_type=jnp.float32)

    theirs = lax.ppermute(project(1 - side).astype(jnp.bfloat16), "head", [(0, 1), (1, 0)])
    return (project(side) + theirs.astype(jnp.float32)).astype(jnp.bfloat16)


def solution(mesh):
    return jax.shard_map(
        functools.partial(shards, mesh.shape["seq"]),
        mesh=mesh,
        in_specs=(
            P(("groups", "seq"), "head", None),
            P(("groups", "seq"), "head", None),
            P(("groups", "seq"), "head", None),
            P(("groups", "seq"), "head", None),
            P("head", None, None),
            P(None, "head", None),
            P(None, "head", None),
            P(None, "head"),
        ),
        out_specs=P(("groups", "seq"), "head"),
        check_vma=False,
    )
```
